32 devices in a mesh: dp: 16 (over z, y, x), tensor: 2 (over core).
Axes of the slice: x: 2, y: 2, z: 4, core: 2. Of those that a mesh axis runs over, the one named last changes fastest.
Arguments:
- encoded: bfloat16 [8192, 1152], P('dp', 'tensor'), may hold values from -9 to 9
- counts: int32 [128], P('dp'), may hold values from 16 to 64
- win_ids: int32 [128, 64], P('dp'), may hold values from 0 to 31, never falling along the last dimension, each value on 1 to 8 neighbouring positions
- dest_seq: int32 [128], P('dp'), may hold values from 0 to 15, as said below
- dest_slot: int32 [128], P('dp'), may hold values from 0 to 7, as said below
- w_first: bfloat16 [1152, 4608], P(None, 'tensor'), may hold values from -0.3125 to 0.3125
- b_first: float32 [4608], P('tensor'), may hold values from -3 to 3
- w_second: bfloat16 [4608, 2304], P('tensor'), may hold values from -0.1875 to 0.1875
- b_second: float32 [2304], P('tensor'), may hold values from -3 to 3
Outputs:
- projected: bfloat16 [4096, 2304], P('dp', 'tensor')
The draws below stay inside these ranges and needn't reach their ends.
Inputs may be any that keep to these rules, and one draw needn't show every extreme that they name: `dest_seq`: every sequence receives exactly 8 samples, no two of them from the same index of dp. `dest_slot`: the samples that one sequence receives have distinct block offsets.
All inputs are finite; a program needn't handle non-finite values.
Results may differ from the reference program's by a relative error of at most 0.009.
Values may be sent and summed in bfloat16 or wider, within the bound.
No kernel may reach another device: no remote copies, remote signals or barrier semaphores. Data moves between devices by JAX's collectives and lax.ppermute only.
A program may use at most 128 MiB of HBM per device.

```python
import math
import jax
import jax.numpy as jnp
import numpy as np
from jax import lax

F = 1152
H = 4608
E = 2304
CAP = 64
BLOCK = 32
MOST = 8
SAMP_DEV = 8
SAMPLES = 128
N_TENSOR = 2


def routing_tables(key):
    base = jax.random.fold_in(key, 11)
    key_outer, key_inner, key_shift, key_slots = jax.random.split(base, 4)
    groups = SAMPLES // SAMP_DEV
    outer_perm = jax.random.permutation(key_outer, groups)
    inner_perm = jax.random.permutation(key_inner, groups)
    shifts = jax.random.permutation(key_shift, groups)[:SAMP_DEV]
    sequence = outer_perm[(inner_perm[:, None] + shifts[None, :]) % groups]
    slot_table = jax.vmap(lambda single: jax.random.permutation(single, SAMP_DEV))(jax.random.split(key_slots, groups))
    slot_ids = slot_table[sequence, jnp.arange(SAMP_DEV)[None, :]]
    return (sequence.reshape(-1).astype(jnp.int32), slot_ids.reshape(-1).astype(jnp.int32))


def draw_dest_seq(key, part):
    return routing_tables(key)[0]


def draw_dest_slot(key, part):
    return routing_tables(key)[1]


def touch_ends(array, rng, least, largest):
    spot = [jax.random.randint(jax.random.fold_in(rng, axis), (), 0, length) for axis, length in enumerate(array.shape)]
    longest = array.shape.index(max(array.shape))
    beside = spot[:longest] + [(spot[longest] + 1) % array.shape[longest]] + spot[longest + 1:]
    return array.at[tuple(spot)].set(least).at[tuple(beside)].set(largest)


def with_spikes(result, stream_key, source, target, blocks, factor):
    owner, partner = [(jnp.arange(result.shape[dim]) // (result.shape[dim] // blocks)).reshape([-1 if axis == dim else 1 for axis in range(result.ndim)]) for dim in (source, target)]
    chosen = jax.random.permutation(stream_key, blocks)[partner]
    strong = (owner == chosen) | (owner == (partner + blocks // 2) % blocks)
    return jnp.where(strong, factor * result, result)


def shard_levels(key, dims, pieces, low, top_value):
    loudness = 1.0
    for dim, blocks in pieces:
        heights = jax.random.uniform(jax.random.fold_in(jax.random.fold_in(key, 6), dim), (blocks,), jnp.float32, low / len(pieces), top_value / len(pieces))
        loudness = loudness * jnp.repeat(jnp.exp(heights), dims[dim] // blocks).reshape((-1,) + (1,) * (len(dims) - 1 - dim))
    return loudness


def length_profile(count, total, most, lean):
    portions = [(1 << 20) // math.isqrt(rank ** lean) + 1 for rank in range(2, count + 1)]
    rest, given = total - most - (count - 1), [1] * (count - 1)
    while rest > 0:
        free = [i for i in range(count - 1) if given[i] < most]
        mass, remaining = sum([portions[i] for i in free]), rest
        for i in free:
            more = min(most - given[i], max(1, remaining * portions[i] // mass), rest)
            given[i] = given[i] + more
            rest = rest - more
    return np.array([most] + given)


def uneven(key, count, total, most, lean):
    if count == 2:
        one = jax.random.randint(key, (), max(1, total - most), min(most, total - 1) + 1)
        return jnp.stack([one, total - one])
    sizes = jnp.asarray(length_profile(count, total, most, lean), jnp.int32)
    pairs = (count - 1) // 2
    donor, sink = sizes[1:1 + 2 * pairs:2], sizes[2:2 + 2 * pairs:2]
    margin = jnp.minimum(donor - 1, most - sink)
    shifted = jax.random.randint(jax.random.fold_in(key, 1), (pairs,), 0, 1 << 20) % (margin + 1)
    sizes = sizes.at[1:1 + 2 * pairs:2].set(donor - shifted).at[2:2 + 2 * pairs:2].set(sink + shifted)
    return sizes[jax.random.permutation(jax.random.fold_in(key, 2), count)]


def bell_draw(own_key, shape, scale, reach, cuts=(), kind=jnp.bfloat16):
    loudness = shard_levels(own_key, shape, cuts, -0.22, 0.18) if cuts else 1.0
    drawn = jax.random.normal(own_key, shape, jnp.float32) * scale * loudness
    return jnp.minimum(jnp.maximum(drawn, -reach), reach).astype(kind)


def heavy_noise(rng, shape, spread, bound, cuts, heavy, held_as=jnp.bfloat16):
    drawn = spread * jax.random.normal(rng, shape, jnp.float32)
    if cuts:
        drawn = drawn * shard_levels(rng, shape, cuts, -0.22, 0.18)
    return jnp.clip(with_spikes(drawn, jax.random.fold_in(rng, 3), *heavy), -bound, bound).astype(held_as)


def setup_inputs(seed: int = 0) -> dict:
    streams_of = jax.random.split(jax.random.key(seed), 10)
    return {
        "encoded": bell_draw(streams_of[0], (SAMPLES * CAP, F), 1.5, 9.0, ((0, 16), (1, 2))),
        "counts": touch_ends(jax.random.randint(streams_of[1], (SAMPLES,), CAP // 4, CAP + 1), jax.random.fold_in(streams_of[1], 1), CAP // 4, CAP).astype(jnp.int32),
        "win_ids": jax.vmap(lambda own: jnp.searchsorted(jnp.cumsum(uneven(own, BLOCK, CAP, MOST, 1)), jnp.arange(CAP), side="right"))(jax.random.split(streams_of[2], SAMPLES)).reshape((SAMPLES, CAP)).astype(jnp.int32),
        "dest_seq": draw_dest_seq(jax.random.fold_in(streams_of[9], 71), 0),
        "dest_slot": draw_dest_slot(jax.random.fold_in(streams_of[9], 71), 0),
        "w_first": bell_draw(streams_of[5], (F, H), (F // 3) ** -0.5, 0.3125, ((1, 2),)),
        "b_first": bell_draw(streams_of[6], (H,), 0.5, 3.0, ((0, 2),), jnp.float32),
        "w_second": heavy_noise(streams_of[7], (H, E), (H // 2) ** -0.5, 0.1875, ((0, 2),), (0, 1, 2, 2.0)),
        "b_second": bell_draw(streams_of[8], (E,), 0.5, 3.0, ((0, 2),), jnp.float32),
    }


def reference(encoded, counts, win_ids, dest_seq, dest_slot, w_first, b_first, w_second, b_second):
    tokens = encoded.reshape(SAMPLES, CAP, F)
    positions = jnp.arange(CAP, dtype=jnp.int32)
    ids_live = jnp.where(positions[None, :] < counts[:, None], win_ids, -1)
    windows = jnp.arange(BLOCK, dtype=jnp.int32)
    onehot = (ids_live[:, None, :] == windows[None, :, None]).astype(jnp.float32)
    number = jnp.sum(onehot, axis=2)
    totals = jnp.einsum("nwc,ncf->nwf", onehot, tokens.astype(jnp.float32))
    pooled = (totals / jnp.maximum(number, 1.0)[:, :, None]).astype(jnp.bfloat16)
    position = (dest_seq * SAMP_DEV + dest_slot).astype(jnp.int32)
    packed = jnp.zeros((SAMPLES, BLOCK, F), jnp.bfloat16).at[position].set(pooled)
    packed = packed.reshape(SAMPLES * BLOCK, F)
    preact = jnp.dot(packed, w_first, preferred_element_type=jnp.float32) + b_first
    hidden = jax.nn.gelu(preact, approximate=True).astype(jnp.bfloat16)
    quota_size = H // N_TENSOR
    running = jnp.zeros((SAMPLES * BLOCK, E), jnp.float32)
    for member in range(N_TENSOR):
        portion = jnp.dot(hidden[:, member * quota_size:(member + 1) * quota_size],
                          w_second[member * quota_size:(member + 1) * quota_size],
                          preferred_element_type=jnp.float32).astype(jnp.bfloat16)
        portion = lax.optimization_barrier(portion)
        running = running + portion.astype(jnp.float32)
    return (running + b_second).astype(jnp.bfloat16)
```

```python
import functools

import jax
import jax.numpy as jnp
from jax import lax
from jax.experimental import pallas as pl
from jax.experimental.pallas import tpu as pltpu
from jax.sharding import PartitionSpec as P

BLOCK = 32
LANES = 128
HALF = LANES // 2
NOTE = 8
F32, BF16, I32 = jnp.float32, jnp.bfloat16, jnp.int32
VMEM = pl.BlockSpec(memory_space=pltpu.VMEM)
SMEM = pl.BlockSpec(memory_space=pltpu.SMEM)
ANY = pl.BlockSpec(memory_space=pl.ANY)
HBM = pl.BlockSpec(memory_space=pltpu.HBM)
NT = (((1,), (1,)), ((), ()))
MIB = 1 << 20


def iota(shape, dim):
    return lax.broadcasted_iota(I32, shape, dim)


def params(mib):
    return pltpu.CompilerParams(vmem_limit_bytes=mib * MIB)


def cost(flops, nbytes):
    return pl.CostEstimate(flops=int(flops), bytes_accessed=int(nbytes), transcendentals=0)


def block_rows(features):
    full, rest = divmod(features, LANES)
    assert rest in (0, HALF)
    rows = full * BLOCK + (BLOCK // 2 if rest else 0)
    return full, rest, rows


def pool_kernel(counts, seq, slot, win, enc, out):
    samples, cap = win.shape
    features, tokens = enc.shape
    groups = out.shape[0]
    full, rest, rows = block_rows(features)
    ids = win[...]
    pair = jnp.concatenate([ids, ids], axis=1)
    tiled = jnp.concatenate([pair] * (tokens // (2 * cap)), axis=1)
    lane = iota((samples, tokens), 1)
    mine = (lane // cap) == iota((samples, tokens), 0)
    ids_row = jnp.sum(jnp.where(mine, tiled, 0), axis=0, keepdims=True)
    lane = iota((1, tokens), 1)
    owner, place = lane // cap, lane % cap
    live = jnp.zeros((1, tokens), I32)
    base = jnp.zeros((1, tokens), I32)
    note = jnp.zeros((groups, NOTE, LANES), I32)
    target = iota((groups, NOTE, LANES), 0)
    for n in range(samples):
        live = jnp.where(owner == n, counts[n], live)
        base = jnp.where(owner == n, seq[n] * BLOCK, base)
        note = jnp.where(target == seq[n], slot[n] + 1, note)
    key = jnp.where(place < live, base + ids_row, -1)
    out[:, rows:, :] = note.astype(F32).astype(BF16)
    ones = jnp.ones((tokens, LANES), BF16)
    per = min(groups, 16)
    for g in range(0, groups, per):
        hot = (iota((per * BLOCK, tokens), 0) + g * BLOCK == key).astype(F32).astype(BF16)
        number = jnp.dot(hot, ones, preferred_element_type=F32)
        scale = 1.0 / jnp.maximum(number, 1.0)
        for j in range(full):
            part = enc[j * LANES : (j + 1) * LANES, :]
            got = lax.dot_general(hot, part, NT, preferred_element_type=F32) * scale
            got = got.astype(BF16).reshape(per, BLOCK, LANES)
            out[g : g + per, j * BLOCK : (j + 1) * BLOCK, :] = got
        if rest:
            part = enc[full * LANES :, :]
            part = jnp.concatenate([part, part], axis=0)
            got = lax.dot_general(hot, part, NT, preferred_element_type=F32) * scale
            got = got.reshape(per, BLOCK, LANES)
            low, high = got[:, : BLOCK // 2], got[:, BLOCK // 2 :]
            left = iota(low.shape, 2) < HALF
            out[g : g + per, full * BLOCK : rows, :] = jnp.where(left, low, high).astype(BF16)


def place_kernel(came, out):
    groups = came.shape[0]
    total, features = out.shape
    full, rest, rows = block_rows(features)
    note = came[:, rows : rows + NOTE, :].astype(F32)[:, 0, :].astype(BF16)
    spread = (iota((groups, groups * BLOCK), 1) // BLOCK == iota((groups, groups * BLOCK), 0)).astype(F32).astype(BF16)
    tn = (((0,), (0,)), ((), ()))
    slot_row = lax.dot_general(note, spread, tn, preferred_element_type=F32)[:1, :]
    lane = iota((1, groups * BLOCK), 1)
    key = (slot_row.astype(I32) - 1) * BLOCK + lane % BLOCK
    hot = (iota((total, groups * BLOCK), 0) == key).astype(F32).astype(BF16)
    for j in range(full):
        part = came[:, j * BLOCK : (j + 1) * BLOCK, :].reshape(groups * BLOCK, LANES)
        got = jnp.dot(hot, part, preferred_element_type=F32)
        out[:, j * LANES : (j + 1) * LANES] = got.astype(BF16)
    if rest:
        part = came[:, full * BLOCK : rows, :]
        twice = jnp.concatenate([part, part], axis=1).reshape(groups * BLOCK, LANES)
        got = jnp.dot(hot, twice, preferred_element_type=F32)
        low = iota((total, LANES), 0) % BLOCK < BLOCK // 2
        got = jnp.where(low, got, pltpu.roll(got, HALF, 1))
        out[:, full * LANES :] = got[:, :HALF].astype(BF16)


def fetch_kernel(w1, w2, v1, v2, sems):
    copies = [
        pltpu.make_async_copy(w1, v1, sems.at[0]),
        pltpu.make_async_copy(w2, v2, sems.at[1]),
    ]
    for copy in copies:
        copy.start()
    for copy in copies:
        copy.wait()


def columns(width, most=768):
    step = max(d for d in range(LANES, most + 1, LANES) if width % d == 0)
    return [(c, step) for c in range(0, width, step)]


def first_kernel(own, w, out):
    depth = own.shape[1]
    start = pl.multiple_of(lax.axis_index("tensor") * depth, NOTE)
    for c, n in columns(out.shape[1]):
        out[:, c : c + n] = jnp.dot(own[...], w[pl.ds(start, depth), c : c + n], preferred_element_type=F32)


def hidden_kernel(acc, other, w, b, w2, hidden, part):
    depth = other.shape[1]
    me = lax.axis_index("tensor")
    start = pl.multiple_of((1 - me) * depth, NOTE)
    for c, n in columns(acc.shape[1]):
        got = jnp.dot(other[...], w[pl.ds(start, depth), c : c + n], preferred_element_type=F32)
        got = got + acc[:, c : c + n] + b[:, c : c + n]
        hidden[:, c : c + n] = jax.nn.gelu(got, approximate=True).astype(BF16)
    width = part.shape[1]
    for c, n in columns(width, 384):
        col = pl.multiple_of((1 - me) * width + c, LANES)
        part[:, c : c + n] = jnp.dot(hidden[...], w2[:, pl.ds(col, n)], preferred_element_type=F32).astype(BF16)


def second_kernel(hidden, w2, part):
    width = part.shape[1]
    me = lax.axis_index("tensor")
    for c, n in columns(width, 384):
        col = pl.multiple_of(me * width + c, LANES)
        part[:, c : c + n] = jnp.dot(hidden[...], w2[:, pl.ds(col, n)], preferred_element_type=F32).astype(BF16)


def shards(encoded, counts, win_ids, dest_seq, dest_slot, w_first, b_first, w_second, b_second):
    groups = lax.axis_size("dp")
    samples = counts.shape[0]
    tokens, features = encoded.shape
    hidden_units = w_first.shape[1]
    width = b_second.shape[0]
    rows = block_rows(features)[2] + NOTE
    total = samples * BLOCK
    swap = ((0, 1), (1, 0))

    outgoing = pl.pallas_call(
        pool_kernel,
        out_shape=jax.ShapeDtypeStruct((groups, rows, LANES), BF16),
        in_specs=[SMEM, SMEM, SMEM, VMEM, VMEM],
        out_specs=VMEM,
        compiler_params=params(20),
        cost_estimate=cost(2e10, 6e7),
        name="pool",
    )(counts, dest_seq, dest_slot, win_ids, encoded.T)
    came = lax.all_to_all(outgoing, "dp", split_axis=0, concat_axis=0, tiled=True)
    w1, w2 = w_first, w_second
    own = pl.pallas_call(
        place_kernel,
        out_shape=jax.ShapeDtypeStruct((total, features), BF16),
        in_specs=[VMEM],
        out_specs=VMEM,
        compiler_params=params(20),
        cost_estimate=cost(2 * total * groups * BLOCK * features, 4 * total * features),
        name="place",
    )(came)
    other = lax.ppermute(own, "tensor", swap)
    acc = pl.pallas_call(
        first_kernel,
        out_shape=jax.ShapeDtypeStruct((total, hidden_units), F32),
        in_specs=[VMEM, VMEM],
        out_specs=VMEM,
        compiler_params=params(20),
        cost_estimate=cost(2 * total * features * hidden_units, 4 * total * hidden_units),
        name="first",
    )(own, w1)
    hidden, away = pl.pallas_call(
        hidden_kernel,
        out_shape=(
            jax.ShapeDtypeStruct((total, hidden_units), BF16),
            jax.ShapeDtypeStruct((total, width), BF16),
        ),
        in_specs=[VMEM] * 5,
        out_specs=(VMEM, VMEM),
        compiler_params=params(20),
        cost_estimate=cost(2 * total * (features + width) * hidden_units, 4 * total * hidden_units),
        name="hidden",
    )(acc, other, w1, b_first.reshape(1, -1), w2)
    back = lax.ppermute(away, "tensor", swap)
    kept = pl.pallas_call(
        second_kernel,
        out_shape=jax.ShapeDtypeStruct((total, width), BF16),
        in_specs=[VMEM, VMEM],
        out_specs=VMEM,
        compiler_params=params(20),
        cost_estimate=cost(2 * total * width * hidden_units, 4 * total * hidden_units),
        name="second",
    )(hidden, w2)
    return (kept.astype(F32) + back.astype(F32) + b_second).astype(BF16)


def solution(mesh):
    placed = (
        P("dp", "tensor"),
        P("dp"),
        P("dp", None),
        P("dp"),
        P("dp"),
        P(None, "tensor"),
        P("tensor"),
        P("tensor", None),
        P("tensor"),
    )
    return jax.shard_map(
        shards, mesh=mesh, in_specs=placed, out_specs=P("dp", "tensor"), check_vma=False
    )
```

```python
import math

import jax
import jax.numpy as jnp
from jax import lax
from jax.experimental import pallas as pl
from jax.experimental.pallas import tpu as pltpu
from jax.sharding import PartitionSpec as P

BLOCK = 32
LANES = 128
HALF = LANES // 2
NOTE = 8
F32, BF16, I32 = jnp.float32, jnp.bfloat16, jnp.int32
VMEM = pl.BlockSpec(memory_space=pltpu.VMEM)
SMEM = pl.BlockSpec(memory_space=pltpu.SMEM)
ANY = pl.BlockSpec(memory_space=pl.ANY)
HBM = pl.BlockSpec(memory_space=pltpu.HBM)
NT = (((1,), (1,)), ((), ()))
TILE = 256
GRANT = 20 << 20
POOL_FLOPS, POOL_BYTES = 2e10, 6e7
GELU_A = (2 / math.pi) ** 0.5
GELU_B = 0.044715 * GELU_A


def iota(shape, dim):
    return lax.broadcasted_iota(I32, shape, dim)


def block_rows(features):
    full, rest = divmod(features, LANES)
    assert rest in (0, HALF)
    rows = full * BLOCK + (BLOCK // 2 if rest else 0)
    return full, rest, rows


def load_kernel(counts_in, seq_in, slot_in, win_in, enc_in, key, note, enc, counts, seq, slot, win, small, large):
    samples, cap = win.shape
    tokens = enc.shape[1]
    groups = note.shape[0]
    smalls = [
        pltpu.make_async_copy(a, b, small.at[i])
        for i, (a, b) in enumerate(((win_in, win), (counts_in, counts), (seq_in, seq), (slot_in, slot)))
    ]
    tall = pltpu.make_async_copy(enc_in, enc, large)
    for copy in smalls:
        copy.start()
    tall.start()
    for copy in smalls:
        copy.wait()
    ids = win[...]
    pair = jnp.concatenate([ids, ids], axis=1)
    tiled = jnp.concatenate([pair] * (tokens // (2 * cap)), axis=1)
    lane = iota((samples, tokens), 1)
    mine = (lane // cap) == iota((samples, tokens), 0)
    ids_row = jnp.sum(jnp.where(mine, tiled, 0), axis=0, keepdims=True)
    lane = iota((1, tokens), 1)
    owner, place = lane // cap, lane % cap
    live = jnp.zeros((1, tokens), I32)
    base = jnp.zeros((1, tokens), I32)
    notes = jnp.zeros((groups, NOTE, LANES), I32)
    target = iota((groups, NOTE, LANES), 0)
    for n in range(samples):
        live = jnp.where(owner == n, counts[n], live)
        base = jnp.where(owner == n, seq[n] * BLOCK, base)
        notes = jnp.where(target == seq[n], slot[n] + 1, notes)
    key[...] = jnp.where(place < live, base + ids_row, -1)
    note[...] = notes.astype(F32).astype(BF16)
    tall.wait()


def pool_kernel(key, note, enc, out):
    features, tokens = enc.shape
    groups = out.shape[0]
    full, rest, rows = block_rows(features)
    out[:, rows:, :] = note[...]
    ones = jnp.ones((tokens, LANES), BF16)
    per = min(groups, 16)
    for g in range(0, groups, per):
        hot = (iota((per * BLOCK, tokens), 0) + g * BLOCK == key[...]).astype(F32).astype(BF16)
        number = jnp.dot(hot, ones, preferred_element_type=F32)
        scale = 1.0 / jnp.maximum(number, 1.0)
        for j in range(full):
            part = enc[j * LANES : (j + 1) * LANES, :]
            got = lax.dot_general(hot, part, NT, preferred_element_type=F32) * scale
            got = got.astype(BF16).reshape(per, BLOCK, LANES)
            out[g : g + per, j * BLOCK : (j + 1) * BLOCK, :] = got
        if rest:
            part = enc[full * LANES :, :]
            part = jnp.concatenate([part, part], axis=0)
            got = lax.dot_general(hot, part, NT, preferred_element_type=F32) * scale
            got = got.reshape(per, BLOCK, LANES)
            low, high = got[:, : BLOCK // 2], got[:, BLOCK // 2 :]
            left = iota(low.shape, 2) < HALF
            out[g : g + per, full * BLOCK : rows, :] = jnp.where(left, low, high).astype(BF16)


def place_kernel(came, out):
    groups = came.shape[0]
    total, padded = out.shape
    rows = came.shape[1] - NOTE
    full = rows // BLOCK
    each = LANES // BLOCK
    turn = iota((NOTE, LANES), 1) // BLOCK
    keys = []
    for d in range(0, groups, each):
        key = came[d, rows:, :].astype(F32)
        for i in range(1, each):
            key = jnp.where(turn == i, came[d + i, rows:, :].astype(F32), key)
        keys.append(key)
    key = jnp.concatenate(keys, axis=1)[:1].astype(I32)
    key = (key - 1) * BLOCK + iota((1, groups * BLOCK), 1) % BLOCK
    hot = (iota((total, groups * BLOCK), 0) == key).astype(F32).astype(BF16)
    for j in range(full):
        part = came[:, j * BLOCK : (j + 1) * BLOCK, :].reshape(groups * BLOCK, LANES)
        got = jnp.dot(hot, part, preferred_element_type=F32)
        out[:, j * LANES : (j + 1) * LANES] = got.astype(BF16)
    if rows > full * BLOCK:
        part = came[:, full * BLOCK : rows, :]
        twice = jnp.concatenate([part, part], axis=1).reshape(groups * BLOCK, LANES)
        got = jnp.dot(hot, twice, preferred_element_type=F32)
        low = iota((total, LANES), 0) % BLOCK < BLOCK // 2
        left = iota((total, LANES), 1) < HALF
        out[:, full * LANES :] = jnp.where(low == left, got, pltpu.roll(got, HALF, 1)).astype(BF16)


def columns(width, most):
    step = max(d for d in range(LANES, most + 1, LANES) if width % d == 0)
    return [(c, step) for c in range(0, width, step)]


def first_kernel(own, w, out):
    depth = w.shape[0] // 2
    deep = depth // LANES * LANES
    start = pl.multiple_of(lax.axis_index("tensor") * depth, HALF)
    for c, n in columns(out.shape[1], 768):
        out[:, c : c + n] = jnp.dot(own[:, :deep], w[pl.ds(start, deep), c : c + n], preferred_element_type=F32)


def gelu(x):
    inner = x * (GELU_A + GELU_B * (x * x))
    half = 0.5 * x
    return half + half * jnp.tanh(inner)


def hidden_kernel(acc, own, other, w, b, w2, hidden, away, extra):
    me = lax.axis_index("tensor")
    depth = w.shape[0] // 2
    deep = depth // LANES * LANES
    mine = pl.multiple_of(me * depth, HALF)
    theirs = pl.multiple_of((1 - me) * depth, HALF)
    left = other[:, :deep]
    if deep < depth:
        low = iota((other.shape[0], LANES), 1) < HALF
        both = jnp.where(low, own[:, deep:].astype(F32), other[:, deep:].astype(F32)).astype(BF16)
        left = jnp.concatenate([left, both], axis=1)
    for c, n in columns(acc.shape[1], 768):
        right = w[pl.ds(theirs, deep), c : c + n]
        if deep < depth:
            right = jnp.concatenate(
                [right, w[pl.ds(mine + deep, HALF), c : c + n], w[pl.ds(theirs + deep, HALF), c : c + n]], axis=0
            )
        got = jnp.dot(left, right, preferred_element_type=F32)
        got = got + acc[:, c : c + n] + b[:, c : c + n]
        hidden[:, c : c + n] = gelu(got).astype(BF16)
    width = away.shape[1]
    odd = width % TILE
    window = width + odd
    base = (1 - me) * (width - odd)
    ends = []
    for c in range(0, window, TILE):
        col = pl.multiple_of(base + c, LANES)
        got = jnp.dot(hidden[...], w2[:, pl.ds(col, TILE)], preferred_element_type=F32).astype(BF16)
        for h in range(0, TILE, LANES):
            piece = got[:, h : h + LANES]
            if odd and (c + h == 0 or c + h == window - LANES):
                ends.append(piece.astype(F32))
            else:
                at = c + h - LANES * (1 - me) if odd else c + h
                away[:, pl.ds(pl.multiple_of(at, LANES), LANES)] = piece
    if odd:
        at = pl.multiple_of((1 - me) * (width - LANES), LANES)
        away[:, pl.ds(at, LANES)] = jnp.where(me == 0, ends[1], ends[0]).astype(BF16)
        extra[...] = jnp.where(me == 0, ends[0], ends[1]).astype(BF16)


def second_kernel(hidden, w2, part):
    width = w2.shape[1] // 2
    base = lax.axis_index("tensor") * (width + width % TILE)
    for c in range(0, part.shape[1], TILE):
        col = pl.multiple_of(base + c, LANES)
        part[:, c : c + TILE] = jnp.dot(hidden[...], w2[:, pl.ds(col, TILE)], preferred_element_type=F32).astype(BF16)


def final_kernel(part, extra, back, b, out, held, sems):
    me = lax.axis_index("tensor")
    width = out.shape[1]
    odd = width % TILE
    done = part.shape[1]
    copies = []

    def put(at, size, value):
        at = pl.multiple_of(at, LANES)
        total = value + back[:, pl.ds(at, size)].astype(F32) + b[:, pl.ds(at, size)]
        held[:, pl.ds(at, size)] = total.astype(BF16)
        copies.append(
            pltpu.make_async_copy(held.at[:, pl.ds(at, size)], out.at[:, pl.ds(at, size)], sems.at[len(copies)])
        )
        copies[-1].start()

    for c in range(0, done, TILE):
        put(me * odd + c, TILE, part[:, c : c + TILE].astype(F32))
    if odd:
        put((1 - me) * (width - odd), odd, extra[...].astype(F32))
    for copy in copies:
        copy.wait()


def in_hbm(x):
    return pltpu.with_memory_space_constraint(x, pltpu.HBM)


def call(kernel, shapes, specs, out_specs, flops, nbytes, scratch=()):
    return pl.pallas_call(
        kernel,
        out_shape=shapes,
        in_specs=specs,
        out_specs=out_specs,
        scratch_shapes=list(scratch),
        compiler_params=pltpu.CompilerParams(vmem_limit_bytes=GRANT),
        cost_estimate=pl.CostEstimate(flops=int(flops), bytes_accessed=int(nbytes), transcendentals=0),
        name=kernel.__name__.removesuffix("_kernel"),
    )


def shards(encoded, counts, win_ids, dest_seq, dest_slot, w_first, b_first, w_second, b_second):
    groups = lax.axis_size("dp")
    samples = counts.shape[0]
    tokens, features = encoded.shape
    units = w_first.shape[1]
    width = b_second.shape[0]
    full, rest, rows = block_rows(features)
    total = samples * BLOCK
    swap = ((0, 1), (1, 0))
    shape = jax.ShapeDtypeStruct
    dma = pltpu.SemaphoreType.DMA
    ints = pltpu.SMEM((samples,), I32)
    odd = width % TILE
    early = width - odd

    key, note, enc = call(
        load_kernel,
        (pltpu.VMEM((1, tokens), I32), pltpu.VMEM((groups, NOTE, LANES), BF16), pltpu.VMEM((features, tokens), BF16)),
        [HBM] * 5,
        (VMEM, VMEM, VMEM),
        0,
        2 * tokens * features,
        [ints, ints, ints, pltpu.VMEM(win_ids.shape, I32), dma((4,)), dma],
    )(in_hbm(counts), in_hbm(dest_seq), in_hbm(dest_slot), in_hbm(win_ids), in_hbm(encoded.T))
    outgoing = call(
        pool_kernel,
        shape((groups, rows + NOTE, LANES), BF16),
        [VMEM] * 3,
        VMEM,
        POOL_FLOPS,
        POOL_BYTES,
    )(key, note, enc)
    came = lax.all_to_all(outgoing, "dp", split_axis=0, concat_axis=0, tiled=True)
    own = call(
        place_kernel,
        shape((total, (full + (rest > 0)) * LANES), BF16),
        [VMEM],
        VMEM,
        2 * total * groups * BLOCK * features,
        4 * total * features,
    )(came)
    other = lax.ppermute(own, "tensor", swap)
    acc = call(
        first_kernel,
        shape((total, units), F32),
        [VMEM] * 2,
        VMEM,
        2 * total * features * units,
        4 * total * units,
    )(own, w_first)
    hidden, away, extra = call(
        hidden_kernel,
        (shape((total, units), BF16), shape((total, width), BF16), shape((total, LANES), BF16)),
        [VMEM] * 6,
        (VMEM, VMEM, VMEM),
        2 * total * (features + width) * units,
        4 * total * units,
    )(acc, own, other, w_first, b_first.reshape(1, -1), w_second)
    back = lax.ppermute(away, "tensor", swap)
    part = call(
        second_kernel,
        shape((total, early), BF16),
        [VMEM] * 2,
        VMEM,
        2 * total * early * units,
        4 * total * units,
    )(hidden, w_second)
    return call(
        final_kernel,
        shape((total, width), BF16),
        [VMEM] * 4,
        ANY,
        total * width,
        4 * total * width,
        [pltpu.VMEM((total, width), BF16), dma((early // TILE + 1,))],
    )(part, extra, back, b_second.reshape(1, -1))


def solution(mesh):
    placed = (
        P("dp", "tensor"),
        P("dp"),
        P("dp", None),
        P("dp"),
        P("dp"),
        P(None, "tensor"),
        P("tensor"),
        P("tensor", None),
        P("tensor"),
    )
    return jax.shard_map(
        shards, mesh=mesh, in_specs=placed, out_specs=P("dp", "tensor"), check_vma=False
    )
```

```python
import functools
import math

import jax
import jax.numpy as jnp
from jax import lax
from jax.experimental import pallas as pl
from jax.experimental.pallas import tpu as pltpu
from jax.sharding import PartitionSpec as P

BLOCK = 32
LANES = 128
HALF = LANES // 2
NOTE = 8
F32, BF16, I32 = jnp.float32, jnp.bfloat16, jnp.int32
VMEM = pl.BlockSpec(memory_space=pltpu.VMEM)
SMEM = pl.BlockSpec(memory_space=pltpu.SMEM)
ANY = pl.BlockSpec(memory_space=pl.ANY)
HBM = pl.BlockSpec(memory_space=pltpu.HBM)
NT = (((1,), (1,)), ((), ()))
TILE = 256
GRANT = 20 << 20
POOL_FLOPS, POOL_BYTES = 2e10, 6e7
GELU_A = (2 / math.pi) ** 0.5
GELU_B = 0.044715 * GELU_A


def iota(shape, dim):
    return lax.broadcasted_iota(I32, shape, dim)


def block_rows(features):
    full, rest = divmod(features, LANES)
    assert rest in (0, HALF)
    rows = full * BLOCK + (BLOCK // 2 if rest else 0)
    return full, rest, rows


def load_kernel(shift, counts_in, seq_in, slot_in, win_in, enc_in, key, note, enc, counts, seq, slot, win, small, large):
    samples, cap = win.shape
    tokens = enc.shape[1]
    groups = note.shape[0]
    smalls = [
        pltpu.make_async_copy(a, b, small.at[i])
        for i, (a, b) in enumerate(((win_in, win), (counts_in, counts), (seq_in, seq), (slot_in, slot)))
    ]
    tall = pltpu.make_async_copy(enc_in, enc, large)
    for copy in smalls:
        copy.start()
    tall.start()
    for copy in smalls:
        copy.wait()
    ids = win[...]
    pair = jnp.concatenate([ids, ids], axis=1)
    tiled = jnp.concatenate([pair] * (tokens // (2 * cap)), axis=1)
    lane = iota((samples, tokens), 1)
    mine = (lane // cap) == iota((samples, tokens), 0)
    ids_row = jnp.sum(jnp.where(mine, tiled, 0), axis=0, keepdims=True)
    lane = iota((1, tokens), 1)
    owner, place = lane // cap, lane % cap
    live = jnp.zeros((1, tokens), I32)
    base = jnp.zeros((1, tokens), I32)
    notes = jnp.zeros((groups, NOTE, LANES), I32)
    target = iota((groups, NOTE, LANES), 0)
    for n in range(samples):
        goal = seq[n] + shift
        goal = jnp.where(goal >= groups, goal - groups, goal)
        live = jnp.where(owner == n, counts[n], live)
        base = jnp.where(owner == n, goal * BLOCK, base)
        notes = jnp.where(target == goal, slot[n] + 1, notes)
    key[...] = jnp.where(place < live, base + ids_row, -1)
    note[...] = notes.astype(F32).astype(BF16)
    tall.wait()


def pool_kernel(key, note, enc, out):
    features, tokens = enc.shape
    groups = out.shape[0]
    full, rest, rows = block_rows(features)
    out[:, rows:, :] = note[...]
    ones = jnp.ones((tokens, LANES), BF16)
    per = min(groups, 16)
    for g in range(0, groups, per):
        hot = (iota((per * BLOCK, tokens), 0) + g * BLOCK == key[...]).astype(F32).astype(BF16)
        number = jnp.dot(hot, ones, preferred_element_type=F32)
        scale = 1.0 / jnp.maximum(number, 1.0)
        for j in range(full):
            part = enc[j * LANES : (j + 1) * LANES, :]
            got = lax.dot_general(hot, part, NT, preferred_element_type=F32) * scale
            got = got.astype(BF16).reshape(per, BLOCK, LANES)
            out[g : g + per, j * BLOCK : (j + 1) * BLOCK, :] = got
        if rest:
            part = enc[full * LANES :, :]
            part = jnp.concatenate([part, part], axis=0)
            got = lax.dot_general(hot, part, NT, preferred_element_type=F32) * scale
            got = got.reshape(per, BLOCK, LANES)
            low, high = got[:, : BLOCK // 2], got[:, BLOCK // 2 :]
            left = iota(low.shape, 2) < HALF
            out[g : g + per, full * BLOCK : rows, :] = jnp.where(left, low, high).astype(BF16)


def place_kernel(came, out):
    groups = came.shape[0]
    total, padded = out.shape
    rows = came.shape[1] - NOTE
    full = rows // BLOCK
    each = LANES // BLOCK
    turn = iota((NOTE, LANES), 1) // BLOCK
    keys = []
    for d in range(0, groups, each):
        key = came[d, rows:, :].astype(F32)
        for i in range(1, each):
            key = jnp.where(turn == i, came[d + i, rows:, :].astype(F32), key)
        keys.append(key)
    key = jnp.concatenate(keys, axis=1)[:1].astype(I32)
    key = (key - 1) * BLOCK + iota((1, groups * BLOCK), 1) % BLOCK
    hot = (iota((total, groups * BLOCK), 0) == key).astype(F32).astype(BF16)
    for j in range(full):
        part = came[:, j * BLOCK : (j + 1) * BLOCK, :].reshape(groups * BLOCK, LANES)
        got = jnp.dot(hot, part, preferred_element_type=F32)
        out[:, j * LANES : (j + 1) * LANES] = got.astype(BF16)
    if rows > full * BLOCK:
        part = came[:, full * BLOCK : rows, :]
        twice = jnp.concatenate([part, part], axis=1).reshape(groups * BLOCK, LANES)
        got = jnp.dot(hot, twice, preferred_element_type=F32)
        low = iota((total, LANES), 0) % BLOCK < BLOCK // 2
        left = iota((total, LANES), 1) < HALF
        out[:, full * LANES :] = jnp.where(low == left, got, pltpu.roll(got, HALF, 1)).astype(BF16)


def columns(width, most):
    step = max(d for d in range(LANES, most + 1, LANES) if width % d == 0)
    return [(c, step) for c in range(0, width, step)]


def first_kernel(own, w, out):
    depth = w.shape[0] // 2
    deep = depth // LANES * LANES
    start = pl.multiple_of(lax.axis_index("tensor") * depth, HALF)
    for c, n in columns(out.shape[1], 768):
        out[:, c : c + n] = jnp.dot(own[:, :deep], w[pl.ds(start, deep), c : c + n], preferred_element_type=F32)


def gelu(x):
    inner = x * (GELU_A + GELU_B * (x * x))
    half = 0.5 * x
    return half + half * jnp.tanh(inner)


def hidden_kernel(acc, own, other, w, b, w2, hidden, away, extra):
    me = lax.axis_index("tensor")
    depth = w.shape[0] // 2
    deep = depth // LANES * LANES
    mine = pl.multiple_of(me * depth, HALF)
    theirs = pl.multiple_of((1 - me) * depth, HALF)
    left = other[:, :deep]
    if deep < depth:
        low = iota((other.shape[0], LANES), 1) < HALF
        both = jnp.where(low, own[:, deep:].astype(F32), other[:, deep:].astype(F32)).astype(BF16)
        left = jnp.concatenate([left, both], axis=1)
    for c, n in columns(acc.shape[1], 768):
        right = w[pl.ds(theirs, deep), c : c + n]
        if deep < depth:
            right = jnp.concatenate(
                [right, w[pl.ds(mine + deep, HALF), c : c + n], w[pl.ds(theirs + deep, HALF), c : c + n]], axis=0
            )
        got = jnp.dot(left, right, preferred_element_type=F32)
        got = got + acc[:, c : c + n] + b[:, c : c + n]
        hidden[:, c : c + n] = gelu(got).astype(BF16)
    width = away.shape[1]
    odd = width % TILE
    window = width + odd
    base = (1 - me) * (width - odd)
    ends = []
    for c in range(0, window, TILE):
        col = pl.multiple_of(base + c, LANES)
        got = jnp.dot(hidden[...], w2[:, pl.ds(col, TILE)], preferred_element_type=F32).astype(BF16)
        for h in range(0, TILE, LANES):
            piece = got[:, h : h + LANES]
            if odd and (c + h == 0 or c + h == window - LANES):
                ends.append(piece.astype(F32))
            else:
                at = c + h - LANES * (1 - me) if odd else c + h
                away[:, pl.ds(pl.multiple_of(at, LANES), LANES)] = piece
    if odd:
        at = pl.multiple_of((1 - me) * (width - LANES), LANES)
        away[:, pl.ds(at, LANES)] = jnp.where(me == 0, ends[1], ends[0]).astype(BF16)
        extra[...] = jnp.where(me == 0, ends[0], ends[1]).astype(BF16)


def second_kernel(hidden, w2, part):
    width = w2.shape[1] // 2
    base = lax.axis_index("tensor") * (width + width % TILE)
    for c in range(0, part.shape[1], TILE):
        col = pl.multiple_of(base + c, LANES)
        part[:, c : c + TILE] = jnp.dot(hidden[...], w2[:, pl.ds(col, TILE)], preferred_element_type=F32).astype(BF16)


def final_kernel(part, extra, back, b, out, held, sems):
    me = lax.axis_index("tensor")
    width = out.shape[1]
    odd = width % TILE
    done = part.shape[1]
    copies = []

    def put(at, size, value):
        at = pl.multiple_of(at, LANES)
        total = value + back[:, pl.ds(at, size)].astype(F32) + b[:, pl.ds(at, size)]
        held[:, pl.ds(at, size)] = total.astype(BF16)
        copies.append(
            pltpu.make_async_copy(held.at[:, pl.ds(at, size)], out.at[:, pl.ds(at, size)], sems.at[len(copies)])
        )
        copies[-1].start()

    for c in range(0, done, TILE):
        put(me * odd + c, TILE, part[:, c : c + TILE].astype(F32))
    if odd:
        put((1 - me) * (width - odd), odd, extra[...].astype(F32))
    for copy in copies:
        copy.wait()


def in_hbm(x):
    return pltpu.with_memory_space_constraint(x, pltpu.HBM)


def call(kernel, shapes, specs, out_specs, flops, nbytes, scratch=()):
    return pl.pallas_call(
        kernel,
        out_shape=shapes,
        in_specs=specs,
        out_specs=out_specs,
        scratch_shapes=list(scratch),
        compiler_params=pltpu.CompilerParams(vmem_limit_bytes=GRANT),
        cost_estimate=pl.CostEstimate(flops=int(flops), bytes_accessed=int(nbytes), transcendentals=0),
        name=getattr(kernel, "func", kernel).__name__.removesuffix("_kernel"),
    )


def shards(encoded, counts, win_ids, dest_seq, dest_slot, w_first, b_first, w_second, b_second):
    groups = lax.axis_size("dp")
    samples = counts.shape[0]
    tokens, features = encoded.shape
    units = w_first.shape[1]
    width = b_second.shape[0]
    full, rest, rows = block_rows(features)
    total = samples * BLOCK
    swap = ((0, 1), (1, 0))
    shape = jax.ShapeDtypeStruct
    dma = pltpu.SemaphoreType.DMA
    ints = pltpu.SMEM((samples,), I32)
    odd = width % TILE
    early = width - odd
    lead = groups * 3 // 4 - 1
    ring = [[(lead + i) % groups for i in range(groups)]]

    key, note, enc = call(
        functools.partial(load_kernel, groups - lead),
        (pltpu.VMEM((1, tokens), I32), pltpu.VMEM((groups, NOTE, LANES), BF16), pltpu.VMEM((features, tokens), BF16)),
        [HBM] * 5,
        (VMEM, VMEM, VMEM),
        0,
        2 * tokens * features,
        [ints, ints, ints, pltpu.VMEM(win_ids.shape, I32), dma((4,)), dma],
    )(in_hbm(counts), in_hbm(dest_seq), in_hbm(dest_slot), in_hbm(win_ids), in_hbm(encoded.T))
    outgoing = call(
        pool_kernel,
        shape((groups, rows + NOTE, LANES), BF16),
        [VMEM] * 3,
        VMEM,
        POOL_FLOPS,
        POOL_BYTES,
    )(key, note, enc)
    came = lax.all_to_all(outgoing, "dp", split_axis=0, concat_axis=0, tiled=True, axis_index_groups=ring)
    own = call(
        place_kernel,
        shape((total, (full + (rest > 0)) * LANES), BF16),
        [VMEM],
        VMEM,
        2 * total * groups * BLOCK * features,
        4 * total * features,
    )(came)
    other = lax.ppermute(own, "tensor", swap)
    acc = call(
        first_kernel,
        shape((total, units), F32),
        [VMEM] * 2,
        VMEM,
        2 * total * features * units,
        4 * total * units,
    )(own, w_first)
    hidden, away, extra = call(
        hidden_kernel,
        (shape((total, units), BF16), shape((total, width), BF16), shape((total, LANES), BF16)),
        [VMEM] * 6,
        (VMEM, VMEM, VMEM),
        2 * total * (features + width) * units,
        4 * total * units,
    )(acc, own, other, w_first, b_first.reshape(1, -1), w_second)
    back = lax.ppermute(away, "tensor", swap)
    part = call(
        second_kernel,
        shape((total, early), BF16),
        [VMEM] * 2,
        VMEM,
        2 * total * early * units,
        4 * total * units,
    )(hidden, w_second)
    return call(
        final_kernel,
        shape((total, width), BF16),
        [VMEM] * 4,
        ANY,
        total * width,
        4 * total * width,
        [pltpu.VMEM((total, width), BF16), dma((early // TILE + 1,))],
    )(part, extra, back, b_second.reshape(1, -1))


def solution(mesh):
    placed = (
        P("dp", "tensor"),
        P("dp"),
        P("dp", None),
        P("dp"),
        P("dp"),
        P(None, "tensor"),
        P("tensor"),
        P("tensor", None),
        P("tensor"),
    )
    return jax.shard_map(
        shards, mesh=mesh, in_specs=placed, out_specs=P("dp", "tensor"), check_vma=False
    )
```

```python
import functools
import math

import jax
import jax.numpy as jnp
from jax import lax
from jax.experimental import pallas as pl
from jax.experimental.pallas import tpu as pltpu
from jax.sharding import PartitionSpec as P

BLOCK = 32
LANES = 128
HALF = LANES // 2
NOTE = 8
F32, BF16, I32 = jnp.float32, jnp.bfloat16, jnp.int32
VMEM = pl.BlockSpec(memory_space=pltpu.VMEM)
SMEM = pl.BlockSpec(memory_space=pltpu.SMEM)
ANY = pl.BlockSpec(memory_space=pl.ANY)
HBM = pl.BlockSpec(memory_space=pltpu.HBM)
NT = (((1,), (1,)), ((), ()))
TILE = 256
PIECES = 4
GRANT = 20 << 20
POOL_FLOPS, POOL_BYTES = 2e10, 6e7
GELU_A = (2 / math.pi) ** 0.5
GELU_B = 0.044715 * GELU_A


def iota(shape, dim):
    return lax.broadcasted_iota(I32, shape, dim)


def block_rows(features):
    full, rest = divmod(features, LANES)
    assert rest in (0, HALF)
    rows = full * BLOCK + (BLOCK // 2 if rest else 0)
    return full, rest, rows


def load_kernel(shift, counts_in, seq_in, slot_in, win_in, enc_in, hot, note, enc, counts, seq, slot, win, small, large):
    samples, cap = win.shape
    tokens = enc.shape[1]
    groups = note.shape[0]
    smalls = [
        pltpu.make_async_copy(a, b, small.at[i])
        for i, (a, b) in enumerate(((win_in, win), (counts_in, counts), (seq_in, seq), (slot_in, slot)))
    ]
    tall = pltpu.make_async_copy(enc_in, enc, large)
    for copy in smalls:
        copy.start()
    tall.start()
    for copy in smalls:
        copy.wait()
    ids = win[...]
    pair = jnp.concatenate([ids, ids], axis=1)
    tiled = jnp.concatenate([pair] * (tokens // (2 * cap)), axis=1)
    lane = iota((samples, tokens), 1)
    mine = (lane // cap) == iota((samples, tokens), 0)
    ids_row = jnp.sum(jnp.where(mine, tiled, 0), axis=0, keepdims=True)
    lane = iota((1, tokens), 1)
    owner, place = lane // cap, lane % cap
    live = jnp.zeros((1, tokens), I32)
    base = jnp.zeros((1, tokens), I32)
    notes = jnp.zeros((groups, NOTE, LANES), I32)
    target = iota((groups, NOTE, LANES), 0)
    for n in range(samples):
        goal = seq[n] + shift
        goal = jnp.where(goal >= groups, goal - groups, goal)
        live = jnp.where(owner == n, counts[n], live)
        base = jnp.where(owner == n, goal * BLOCK, base)
        notes = jnp.where(target == goal, slot[n] + 1, notes)
    key = jnp.where(place < live, base + ids_row, -1)
    note[...] = notes.astype(F32).astype(BF16)
    rows = min(hot.shape[0], 2 * TILE)
    for r in range(0, hot.shape[0], rows):
        hot[r : r + rows, :] = (iota((rows, tokens), 0) + r == key).astype(F32).astype(BF16)
    tall.wait()


def pool_kernel(hot, note, enc, out):
    features, tokens = enc.shape
    groups = out.shape[0]
    full, rest, rows = block_rows(features)
    out[:, rows:, :] = note[...]
    ones = jnp.ones((LANES, tokens), BF16)
    tail = enc[full * LANES :, :]
    tail = jnp.concatenate([tail, tail, ones] if rest else [ones], axis=0)
    per = min(groups, 16)
    for g in range(0, groups, per):
        pick = hot[g * BLOCK : (g + per) * BLOCK, :]
        last = lax.dot_general(pick, tail, NT, preferred_element_type=F32)
        scale = 1.0 / jnp.maximum(last[:, -LANES:], 1.0)
        if rest:
            got = (last[:, :LANES] * scale).reshape(per, BLOCK, LANES)
            low, high = got[:, : BLOCK // 2], got[:, BLOCK // 2 :]
            left = iota(low.shape, 2) < HALF
            out[g : g + per, full * BLOCK : rows, :] = jnp.where(left, low, high).astype(BF16)
        for c in range(0, full * LANES, TILE):
            n = min(TILE, full * LANES - c)
            both = lax.dot_general(pick, enc[c : c + n, :], NT, preferred_element_type=F32)
            for j in range(0, n, LANES):
                got = (both[:, j : j + LANES] * scale).astype(BF16).reshape(per, BLOCK, LANES)
                at = (c + j) // LANES * BLOCK
                out[g : g + per, at : at + BLOCK, :] = got


def place_kernel(came, out):
    groups = came.shape[0]
    total, padded = out.shape
    rows = came.shape[1] - NOTE
    full = rows // BLOCK
    each = LANES // BLOCK
    turn = iota((NOTE, LANES), 1) // BLOCK
    keys = []
    for d in range(0, groups, each):
        key = came[d, rows:, :].astype(F32)
        for i in range(1, each):
            key = jnp.where(turn == i, came[d + i, rows:, :].astype(F32), key)
        keys.append(key)
    key = jnp.concatenate(keys, axis=1)[:1].astype(I32)
    key = (key - 1) * BLOCK + iota((1, groups * BLOCK), 1) % BLOCK
    hot = (iota((total, groups * BLOCK), 0) == key).astype(F32).astype(BF16)
    for j in range(0, full, 2):
        parts = [came[:, i * BLOCK : (i + 1) * BLOCK, :].reshape(groups * BLOCK, LANES) for i in range(j, min(j + 2, full))]
        got = jnp.dot(hot, jnp.concatenate(parts, axis=1), preferred_element_type=F32)
        out[:, j * LANES : (j + len(parts)) * LANES] = got.astype(BF16)
    if rows > full * BLOCK:
        part = came[:, full * BLOCK : rows, :]
        twice = jnp.concatenate([part, part], axis=1).reshape(groups * BLOCK, LANES)
        got = jnp.dot(hot, twice, preferred_element_type=F32)
        low = iota((total, LANES), 0) % BLOCK < BLOCK // 2
        left = iota((total, LANES), 1) < HALF
        out[:, full * LANES :] = jnp.where(low == left, got, pltpu.roll(got, HALF, 1)).astype(BF16)


def columns(width, most):
    step = max(d for d in range(LANES, most + 1, LANES) if width % d == 0)
    return [(c, step) for c in range(0, width, step)]


def first_kernel(own, w, out):
    depth = w.shape[0] // 2
    deep = depth // LANES * LANES
    start = pl.multiple_of(lax.axis_index("tensor") * depth, HALF)
    for c, n in columns(out.shape[1], 768):
        out[:, c : c + n] = jnp.dot(own[:, :deep], w[pl.ds(start, deep), c : c + n], preferred_element_type=F32)


def gelu(x):
    inner = x * (GELU_A + GELU_B * (x * x))
    half = 0.5 * x
    return half + half * jnp.tanh(inner)


def hidden_kernel(acc, own, other, w, b, w2, hidden, away, extra):
    me = lax.axis_index("tensor")
    depth = w.shape[0] // 2
    deep = depth // LANES * LANES
    mine = pl.multiple_of(me * depth, HALF)
    theirs = pl.multiple_of((1 - me) * depth, HALF)
    left = other[:, :deep]
    if deep < depth:
        low = iota((other.shape[0], LANES), 1) < HALF
        both = jnp.where(low, own[:, deep:].astype(F32), other[:, deep:].astype(F32)).astype(BF16)
        left = jnp.concatenate([left, both], axis=1)
    for c, n in columns(acc.shape[1], 768):
        right = w[pl.ds(theirs, deep), c : c + n]
        if deep < depth:
            right = jnp.concatenate(
                [right, w[pl.ds(mine + deep, HALF), c : c + n], w[pl.ds(theirs + deep, HALF), c : c + n]], axis=0
            )
        got = jnp.dot(left, right, preferred_element_type=F32)
        got = got + acc[:, c : c + n] + b[:, c : c + n]
        hidden[:, c : c + n] = gelu(got).astype(BF16)
    width = away.shape[1]
    odd = width % TILE
    window = width + odd
    base = (1 - me) * (width - odd)
    ends = []
    for c in range(0, window, TILE):
        col = pl.multiple_of(base + c, LANES)
        got = jnp.dot(hidden[...], w2[:, pl.ds(col, TILE)], preferred_element_type=F32).astype(BF16)
        for h in range(0, TILE, LANES):
            piece = got[:, h : h + LANES]
            if odd and (c + h == 0 or c + h == window - LANES):
                ends.append(piece.astype(F32))
            else:
                at = c + h - LANES * (1 - me) if odd else c + h
                away[:, pl.ds(pl.multiple_of(at, LANES), LANES)] = piece
    if odd:
        at = pl.multiple_of((1 - me) * (width - LANES), LANES)
        away[:, pl.ds(at, LANES)] = jnp.where(me == 0, ends[1], ends[0]).astype(BF16)
        extra[...] = jnp.where(me == 0, ends[0], ends[1]).astype(BF16)


def second_kernel(hidden, w2, extra, part):
    width = part.shape[1]
    odd = width % TILE
    me = lax.axis_index("tensor")
    if odd:
        part[:, pl.ds(pl.multiple_of((1 - me) * (width - odd), LANES), odd)] = extra[...]
    for c in range(0, width - odd, TILE):
        col = pl.multiple_of(me * (width + odd) + c, LANES)
        got = jnp.dot(hidden[...], w2[:, pl.ds(col, TILE)], preferred_element_type=F32).astype(BF16)
        part[:, pl.ds(pl.multiple_of(me * odd + c, LANES), TILE)] = got


def final_kernel(part, back, b, out, held, sems):
    pieces = sems.shape[0]
    rows = out.shape[0] // pieces
    copies = []
    for i in range(pieces):
        at = slice(i * rows, (i + 1) * rows)
        held[at, :] = (part[at, :].astype(F32) + back[at, :].astype(F32) + b[...]).astype(BF16)
        copies.append(pltpu.make_async_copy(held.at[at], out.at[at], sems.at[i]))
        copies[-1].start()
    for copy in copies:
        copy.wait()


def in_hbm(x):
    return pltpu.with_memory_space_constraint(x, pltpu.HBM)


def call(kernel, shapes, specs, out_specs, flops, nbytes, scratch=()):
    return pl.pallas_call(
        kernel,
        out_shape=shapes,
        in_specs=specs,
        out_specs=out_specs,
        scratch_shapes=list(scratch),
        compiler_params=pltpu.CompilerParams(vmem_limit_bytes=GRANT),
        cost_estimate=pl.CostEstimate(flops=int(flops), bytes_accessed=int(nbytes), transcendentals=0),
        name=getattr(kernel, "func", kernel).__name__.removesuffix("_kernel"),
    )


def shards(encoded, counts, win_ids, dest_seq, dest_slot, w_first, b_first, w_second, b_second):
    groups = lax.axis_size("dp")
    samples = counts.shape[0]
    tokens, features = encoded.shape
    units = w_first.shape[1]
    width = b_second.shape[0]
    full, rest, rows = block_rows(features)
    total = samples * BLOCK
    swap = ((0, 1), (1, 0))
    shape = jax.ShapeDtypeStruct
    dma = pltpu.SemaphoreType.DMA
    ints = pltpu.SMEM((samples,), I32)
    lead = groups * 3 // 4 - 1
    ring = [[(lead + i) % groups for i in range(groups)]]

    hot, note, enc = call(
        functools.partial(load_kernel, groups - lead),
        (pltpu.VMEM((groups * BLOCK, tokens), BF16), pltpu.VMEM((groups, NOTE, LANES), BF16), pltpu.VMEM((features, tokens), BF16)),
        [HBM] * 5,
        (VMEM, VMEM, VMEM),
        0,
        2 * tokens * features,
        [ints, ints, ints, pltpu.VMEM(win_ids.shape, I32), dma((4,)), dma],
    )(in_hbm(counts), in_hbm(dest_seq), in_hbm(dest_slot), in_hbm(win_ids), in_hbm(encoded.T))
    outgoing = call(
        pool_kernel,
        shape((groups, rows + NOTE, LANES), BF16),
        [VMEM] * 3,
        VMEM,
        POOL_FLOPS,
        POOL_BYTES,
    )(hot, note, enc)
    came = lax.all_to_all(outgoing, "dp", split_axis=0, concat_axis=0, tiled=True, axis_index_groups=ring)
    own = call(
        place_kernel,
        shape((total, (full + (rest > 0)) * LANES), BF16),
        [VMEM],
        VMEM,
        2 * total * groups * BLOCK * features,
        4 * total * features,
    )(came)
    other = lax.ppermute(own, "tensor", swap)
    acc = call(
        first_kernel,
        shape((total, units), F32),
        [VMEM] * 2,
        VMEM,
        2 * total * features * units,
        4 * total * units,
    )(own, w_first)
    hidden, away, extra = call(
        hidden_kernel,
        (shape((total, units), BF16), shape((total, width), BF16), shape((total, LANES), BF16)),
        [VMEM] * 6,
        (VMEM, VMEM, VMEM),
        2 * total * (features + width) * units,
        4 * total * units,
    )(acc, own, other, w_first, b_first.reshape(1, -1), w_second)
    back = lax.ppermute(away, "tensor", swap)
    part = call(
        second_kernel,
        shape((total, width), BF16),
        [VMEM] * 3,
        VMEM,
        2 * total * width * units,
        4 * total * units,
    )(hidden, w_second, extra)
    return call(
        final_kernel,
        shape((total, width), BF16),
        [VMEM] * 3,
        ANY,
        total * width,
        4 * total * width,
        [pltpu.VMEM((total, width), BF16), dma((PIECES,))],
    )(part, back, b_second.reshape(1, -1))


def solution(mesh):
    placed = (
        P("dp", "tensor"),
        P("dp"),
        P("dp", None),
        P("dp"),
        P("dp"),
        P(None, "tensor"),
        P("tensor"),
        P("tensor", None),
        P("tensor"),
    )
    return jax.shard_map(
        shards, mesh=mesh, in_specs=placed, out_specs=P("dp", "tensor"), check_vma=False
    )
```

```python
import functools
import math

import jax
import jax.numpy as jnp
from jax import lax
from jax.experimental import pallas as pl
from jax.experimental.pallas import tpu as pltpu
from jax.sharding import PartitionSpec as P

BLOCK = 32
LANES = 128
HALF = LANES // 2
NOTE = 2
F32, BF16, I32 = jnp.float32, jnp.bfloat16, jnp.int32
VMEM = pl.BlockSpec(memory_space=pltpu.VMEM)
SMEM = pl.BlockSpec(memory_space=pltpu.SMEM)
ANY = pl.BlockSpec(memory_space=pl.ANY)
HBM = pl.BlockSpec(memory_space=pltpu.HBM)
NT = (((1,), (1,)), ((), ()))
TILE = 256
PIECES = 4
GRANT = 20 << 20
POOL_FLOPS, POOL_BYTES = 2e10, 6e7
GELU_A = (2 / math.pi) ** 0.5
GELU_B = 0.044715 * GELU_A


def iota(shape, dim):
    return lax.broadcasted_iota(I32, shape, dim)


def block_rows(features):
    full, rest = divmod(features, LANES)
    assert rest in (0, HALF)
    rows = full * BLOCK + (BLOCK // 2 if rest else 0)
    return full, rest, rows


def load_kernel(shift, counts_in, seq_in, slot_in, win_in, enc_in, hot, note, enc, counts, seq, slot, win, small, large):
    samples, cap = win.shape
    tokens = enc.shape[1]
    groups = note.shape[0] // NOTE
    smalls = [
        pltpu.make_async_copy(a, b, small.at[i])
        for i, (a, b) in enumerate(((win_in, win), (counts_in, counts), (seq_in, seq), (slot_in, slot)))
    ]
    tall = pltpu.make_async_copy(enc_in, enc, large)
    for copy in smalls:
        copy.start()
    tall.start()
    for copy in smalls:
        copy.wait()
    ids = win[...]
    pair = jnp.concatenate([ids, ids], axis=1)
    tiled = jnp.concatenate([pair] * (tokens // (2 * cap)), axis=1)
    lane = iota((samples, tokens), 1)
    mine = (lane // cap) == iota((samples, tokens), 0)
    ids_row = jnp.sum(jnp.where(mine, tiled, 0), axis=0, keepdims=True)
    lane = iota((1, tokens), 1)
    owner, place = lane // cap, lane % cap
    live = jnp.zeros((1, tokens), I32)
    base = jnp.zeros((1, tokens), I32)
    notes = jnp.zeros(note.shape, I32)
    target = iota(note.shape, 0) // NOTE
    for n in range(samples):
        goal = seq[n] + shift
        goal = jnp.where(goal >= groups, goal - groups, goal)
        live = jnp.where(owner == n, counts[n], live)
        base = jnp.where(owner == n, goal * BLOCK, base)
        notes = jnp.where(target == goal, slot[n] + 1, notes)
    key = jnp.where(place < live, base + ids_row, -1)
    note[...] = notes.astype(F32).astype(BF16)
    rows = min(hot.shape[0], 2 * TILE)
    for r in range(0, hot.shape[0], rows):
        hot[r : r + rows, :] = (iota((rows, tokens), 0) + r == key).astype(F32).astype(BF16)
    tall.wait()


def pool_kernel(hot, note, enc, out):
    features, tokens = enc.shape
    full, rest, rows = block_rows(features)
    pitch = rows + NOTE
    groups = out.shape[0] // pitch
    ones = jnp.ones((LANES, tokens), BF16)
    tail = enc[full * LANES :, :]
    tail = jnp.concatenate([tail, tail, ones] if rest else [ones], axis=0)
    for g in range(groups):
        out[g * pitch + rows : (g + 1) * pitch, :] = note[g * NOTE : (g + 1) * NOTE, :]
    per = min(groups, 16)
    for g in range(0, groups, per):
        pick = hot[g * BLOCK : (g + per) * BLOCK, :]
        last = lax.dot_general(pick, tail, NT, preferred_element_type=F32)
        scale = 1.0 / jnp.maximum(last[:, -LANES:], 1.0)
        if rest:
            got = (last[:, :LANES] * scale).reshape(per, BLOCK, LANES)
            low, high = got[:, : BLOCK // 2], got[:, BLOCK // 2 :]
            left = iota(low.shape, 2) < HALF
            got = jnp.where(left, low, high).astype(BF16)
            for i in range(per):
                at = (g + i) * pitch + full * BLOCK
                out[at : at + BLOCK // 2, :] = got[i]
        for c in range(0, full * LANES, TILE):
            n = min(TILE, full * LANES - c)
            both = lax.dot_general(pick, enc[c : c + n, :], NT, preferred_element_type=F32)
            for j in range(0, n, LANES):
                got = (both[:, j : j + LANES] * scale).astype(BF16)
                for i in range(per):
                    at = (g + i) * pitch + (c + j) // LANES * BLOCK
                    out[at : at + BLOCK, :] = got[i * BLOCK : (i + 1) * BLOCK]


def place_kernel(came, out, *, groups):
    total, padded = out.shape
    pitch = came.shape[0] // groups
    rows = pitch - NOTE
    full = rows // BLOCK
    each = LANES // BLOCK
    turn = iota((1, LANES), 1) // BLOCK
    keys = []
    for d in range(0, groups, each):
        ends = [came[(d + i) * pitch + rows : (d + i + 1) * pitch, :].astype(F32)[:1] for i in range(each)]
        key = ends[0]
        for i in range(1, each):
            key = jnp.where(turn == i, ends[i], key)
        keys.append(key)
    key = jnp.concatenate(keys, axis=1).astype(I32)
    key = (key - 1) * BLOCK + iota((1, groups * BLOCK), 1) % BLOCK
    hot = (iota((total, groups * BLOCK), 0) == key).astype(F32).astype(BF16)

    def strip(first, size):
        return [came[d * pitch + first : d * pitch + first + size, :] for d in range(groups)]

    for j in range(0, full, 2):
        parts = [jnp.concatenate(strip(i * BLOCK, BLOCK), axis=0) for i in range(j, min(j + 2, full))]
        got = jnp.dot(hot, jnp.concatenate(parts, axis=1), preferred_element_type=F32)
        out[:, j * LANES : (j + len(parts)) * LANES] = got.astype(BF16)
    if rows > full * BLOCK:
        twice = jnp.concatenate([x for part in strip(full * BLOCK, BLOCK // 2) for x in (part, part)], axis=0)
        got = jnp.dot(hot, twice, preferred_element_type=F32)
        low = iota((total, LANES), 0) % BLOCK < BLOCK // 2
        left = iota((total, LANES), 1) < HALF
        out[:, full * LANES :] = jnp.where(low == left, got, pltpu.roll(got, HALF, 1)).astype(BF16)


def columns(width, most):
    step = max(d for d in range(LANES, most + 1, LANES) if width % d == 0)
    return [(c, step) for c in range(0, width, step)]


def first_kernel(own, w, out):
    depth = w.shape[0] // 2
    deep = depth // LANES * LANES
    start = pl.multiple_of(lax.axis_index("tensor") * depth, HALF)
    for c, n in columns(out.shape[1], 768):
        out[:, c : c + n] = jnp.dot(own[:, :deep], w[pl.ds(start, deep), c : c + n], preferred_element_type=F32)


def gelu(x):
    inner = x * (GELU_A + GELU_B * (x * x))
    half = 0.5 * x
    return half + half * jnp.tanh(inner)


def hidden_kernel(acc, own, other, w, b, w2, hidden, away, extra):
    me = lax.axis_index("tensor")
    depth = w.shape[0] // 2
    deep = depth // LANES * LANES
    mine = pl.multiple_of(me * depth, HALF)
    theirs = pl.multiple_of((1 - me) * depth, HALF)
    left = other[:, :deep]
    if deep < depth:
        low = iota((other.shape[0], LANES), 1) < HALF
        both = jnp.where(low, own[:, deep:].astype(F32), other[:, deep:].astype(F32)).astype(BF16)
        left = jnp.concatenate([left, both], axis=1)
    for c, n in columns(acc.shape[1], 768):
        right = w[pl.ds(theirs, deep), c : c + n]
        if deep < depth:
            right = jnp.concatenate(
                [right, w[pl.ds(mine + deep, HALF), c : c + n], w[pl.ds(theirs + deep, HALF), c : c + n]], axis=0
            )
        got = jnp.dot(left, right, preferred_element_type=F32)
        got = got + acc[:, c : c + n] + b[:, c : c + n]
        hidden[:, c : c + n] = gelu(got).astype(BF16)
    width = away.shape[1]
    odd = width % TILE
    window = width + odd
    base = (1 - me) * (width - odd)
    ends = []
    for c in range(0, window, TILE):
        col = pl.multiple_of(base + c, LANES)
        got = jnp.dot(hidden[...], w2[:, pl.ds(col, TILE)], preferred_element_type=F32).astype(BF16)
        for h in range(0, TILE, LANES):
            piece = got[:, h : h + LANES]
            if odd and (c + h == 0 or c + h == window - LANES):
                ends.append(piece.astype(F32))
            else:
                at = c + h - LANES * (1 - me) if odd else c + h
                away[:, pl.ds(pl.multiple_of(at, LANES), LANES)] = piece
    if odd:
        at = pl.multiple_of((1 - me) * (width - LANES), LANES)
        away[:, pl.ds(at, LANES)] = jnp.where(me == 0, ends[1], ends[0]).astype(BF16)
        extra[...] = jnp.where(me == 0, ends[0], ends[1]).astype(BF16)


def second_kernel(hidden, w2, extra, part):
    width = part.shape[1]
    odd = width % TILE
    me = lax.axis_index("tensor")
    if odd:
        part[:, pl.ds(pl.multiple_of((1 - me) * (width - odd), LANES), odd)] = extra[...]
    for c in range(0, width - odd, TILE):
        col = pl.multiple_of(me * (width + odd) + c, LANES)
        got = jnp.dot(hidden[...], w2[:, pl.ds(col, TILE)], preferred_element_type=F32).astype(BF16)
        part[:, pl.ds(pl.multiple_of(me * odd + c, LANES), TILE)] = got


def final_kernel(part, back, b, out, held, sems):
    pieces = sems.shape[0]
    rows = out.shape[0] // pieces
    copies = []
    for i in range(pieces):
        at = slice(i * rows, (i + 1) * rows)
        held[at, :] = (part[at, :].astype(F32) + back[at, :].astype(F32) + b[...]).astype(BF16)
        copies.append(pltpu.make_async_copy(held.at[at], out.at[at], sems.at[i]))
        copies[-1].start()
    for copy in copies:
        copy.wait()


def in_hbm(x):
    return pltpu.with_memory_space_constraint(x, pltpu.HBM)


def call(kernel, shapes, specs, out_specs, flops, nbytes, scratch=()):
    return pl.pallas_call(
        kernel,
        out_shape=shapes,
        in_specs=specs,
        out_specs=out_specs,
        scratch_shapes=list(scratch),
        compiler_params=pltpu.CompilerParams(vmem_limit_bytes=GRANT),
        cost_estimate=pl.CostEstimate(flops=int(flops), bytes_accessed=int(nbytes), transcendentals=0),
        name=getattr(kernel, "func", kernel).__name__.removesuffix("_kernel"),
    )


def shards(encoded, counts, win_ids, dest_seq, dest_slot, w_first, b_first, w_second, b_second):
    groups = lax.axis_size("dp")
    samples = counts.shape[0]
    tokens, features = encoded.shape
    units = w_first.shape[1]
    width = b_second.shape[0]
    full, rest, rows = block_rows(features)
    total = samples * BLOCK
    swap = ((0, 1), (1, 0))
    shape = jax.ShapeDtypeStruct
    dma = pltpu.SemaphoreType.DMA
    ints = pltpu.SMEM((samples,), I32)
    lead = groups * 3 // 4 - 1
    ring = [[(lead + i) % groups for i in range(groups)]]

    hot, note, enc = call(
        functools.partial(load_kernel, groups - lead),
        (pltpu.VMEM((groups * BLOCK, tokens), BF16), pltpu.VMEM((groups * NOTE, LANES), BF16), pltpu.VMEM((features, tokens), BF16)),
        [HBM] * 5,
        (VMEM, VMEM, VMEM),
        0,
        2 * tokens * features,
        [ints, ints, ints, pltpu.VMEM(win_ids.shape, I32), dma((4,)), dma],
    )(in_hbm(counts), in_hbm(dest_seq), in_hbm(dest_slot), in_hbm(win_ids), in_hbm(encoded.T))
    outgoing = call(
        pool_kernel,
        shape((groups * (rows + NOTE), LANES), BF16),
        [VMEM] * 3,
        VMEM,
        POOL_FLOPS,
        POOL_BYTES,
    )(hot, note, enc)
    outgoing = outgoing.reshape(groups, -1, NOTE, LANES)
    came = lax.all_to_all(outgoing, "dp", split_axis=0, concat_axis=0, tiled=True, axis_index_groups=ring)
    came = came.reshape(-1, LANES)
    own = call(
        functools.partial(place_kernel, groups=groups),
        shape((total, (full + (rest > 0)) * LANES), BF16),
        [VMEM],
        VMEM,
        2 * total * groups * BLOCK * features,
        4 * total * features,
    )(came)
    other = lax.ppermute(own, "tensor", swap)
    acc = call(
        first_kernel,
        shape((total, units), F32),
        [VMEM] * 2,
        VMEM,
        2 * total * features * units,
        4 * total * units,
    )(own, w_first)
    hidden, away, extra = call(
        hidden_kernel,
        (shape((total, units), BF16), shape((total, width), BF16), shape((total, LANES), BF16)),
        [VMEM] * 6,
        (VMEM, VMEM, VMEM),
        2 * total * (features + width) * units,
        4 * total * units,
    )(acc, own, other, w_first, b_first.reshape(1, -1), w_second)
    back = lax.ppermute(away, "tensor", swap)
    part = call(
        second_kernel,
        shape((total, width), BF16),
        [VMEM] * 3,
        VMEM,
        2 * total * width * units,
        4 * total * units,
    )(hidden, w_second, extra)
    return call(
        final_kernel,
        shape((total, width), BF16),
        [VMEM] * 3,
        ANY,
        total * width,
        4 * total * width,
        [pltpu.VMEM((total, width), BF16), dma((PIECES,))],
    )(part, back, b_second.reshape(1, -1))


def solution(mesh):
    placed = (
        P("dp", "tensor"),
        P("dp"),
        P("dp", None),
        P("dp"),
        P("dp"),
        P(None, "tensor"),
        P("tensor"),
        P("tensor", None),
        P("tensor"),
    )
    return jax.shard_map(
        shards, mesh=mesh, in_specs=placed, out_specs=P("dp", "tensor"), check_vma=False
    )
```

```python
import functools
import math

import jax
import jax.numpy as jnp
from jax import lax
from jax.experimental import pallas as pl
from jax.experimental.pallas import tpu as pltpu
from jax.sharding import PartitionSpec as P

BLOCK = 32
LANES = 128
HALF = LANES // 2
NOTE = 2
F32, BF16, I32 = jnp.float32, jnp.bfloat16, jnp.int32
VMEM = pl.BlockSpec(memory_space=pltpu.VMEM)
SMEM = pl.BlockSpec(memory_space=pltpu.SMEM)
ANY = pl.BlockSpec(memory_space=pl.ANY)
HBM = pl.BlockSpec(memory_space=pltpu.HBM)
NT = (((1,), (1,)), ((), ()))
TILE = 256
PIECES = 8
GRANT = 20 << 20
POOL_FLOPS, POOL_BYTES = 2e10, 6e7
GELU_A = (2 / math.pi) ** 0.5
GELU_B = 0.044715 * GELU_A


def iota(shape, dim):
    return lax.broadcasted_iota(I32, shape, dim)


def block_rows(features):
    full, rest = divmod(features, LANES)
    assert rest in (0, HALF)
    rows = full * BLOCK + (BLOCK // 2 if rest else 0)
    return full, rest, rows


def load_kernel(shift, counts_in, seq_in, slot_in, win_in, enc_in, hot, note, enc, counts, seq, slot, win, small, large):
    samples, cap = win.shape
    tokens = enc.shape[1]
    groups = note.shape[0] // NOTE
    smalls = [
        pltpu.make_async_copy(a, b, small.at[i])
        for i, (a, b) in enumerate(((win_in, win), (counts_in, counts), (seq_in, seq), (slot_in, slot)))
    ]
    tall = pltpu.make_async_copy(enc_in, enc, large)
    for copy in smalls:
        copy.start()
    tall.start()
    for copy in smalls:
        copy.wait()
    ids = win[...]
    pair = jnp.concatenate([ids, ids], axis=1)
    tiled = jnp.concatenate([pair] * (tokens // (2 * cap)), axis=1)
    lane = iota((samples, tokens), 1)
    mine = (lane // cap) == iota((samples, tokens), 0)
    ids_row = jnp.sum(jnp.where(mine, tiled, 0), axis=0, keepdims=True)
    lane = iota((1, tokens), 1)
    owner, place = lane // cap, lane % cap
    live = jnp.zeros((1, tokens), I32)
    base = jnp.zeros((1, tokens), I32)
    notes = jnp.zeros(note.shape, I32)
    target = iota(note.shape, 0) // NOTE
    for n in range(samples):
        goal = seq[n] + shift
        goal = jnp.where(goal >= groups, goal - groups, goal)
        live = jnp.where(owner == n, counts[n], live)
        base = jnp.where(owner == n, goal * BLOCK, base)
        notes = jnp.where(target == goal, slot[n] + 1, notes)
    key = jnp.where(place < live, base + ids_row, -1)
    note[...] = notes.astype(F32).astype(BF16)
    rows = min(hot.shape[0], 2 * TILE)
    for r in range(0, hot.shape[0], rows):
        hot[r : r + rows, :] = (iota((rows, tokens), 0) + r == key).astype(F32).astype(BF16)
    tall.wait()


def pool_kernel(hot, note, enc, out):
    features, tokens = enc.shape
    full, rest, rows = block_rows(features)
    pitch = rows + NOTE
    groups = out.shape[0] // pitch
    ones = jnp.ones((LANES, tokens), BF16)
    tail = enc[full * LANES :, :]
    tail = jnp.concatenate([tail, tail, ones] if rest else [ones], axis=0)
    for g in range(groups):
        out[g * pitch + rows : (g + 1) * pitch, :] = note[g * NOTE : (g + 1) * NOTE, :]
    per = min(groups, 16)
    for g in range(0, groups, per):
        pick = hot[g * BLOCK : (g + per) * BLOCK, :]
        last = lax.dot_general(pick, tail, NT, preferred_element_type=F32)
        scale = 1.0 / jnp.maximum(last[:, -LANES:], 1.0)
        if rest:
            got = (last[:, :LANES] * scale).reshape(per, BLOCK, LANES)
            low, high = got[:, : BLOCK // 2], got[:, BLOCK // 2 :]
            left = iota(low.shape, 2) < HALF
            got = jnp.where(left, low, high).astype(BF16)
            for i in range(per):
                at = (g + i) * pitch + full * BLOCK
                out[at : at + BLOCK // 2, :] = got[i]
        for c in range(0, full * LANES, TILE):
            n = min(TILE, full * LANES - c)
            both = lax.dot_general(pick, enc[c : c + n, :], NT, preferred_element_type=F32)
            for j in range(0, n, LANES):
                got = (both[:, j : j + LANES] * scale).astype(BF16)
                for i in range(per):
                    at = (g + i) * pitch + (c + j) // LANES * BLOCK
                    out[at : at + BLOCK, :] = got[i * BLOCK : (i + 1) * BLOCK]


def place_kernel(came, out, *, groups):
    total, padded = out.shape
    pitch = came.shape[0] // groups
    rows = pitch - NOTE
    full = rows // BLOCK
    each = LANES // BLOCK
    turn = iota((1, LANES), 1) // BLOCK
    keys = []
    for d in range(0, groups, each):
        ends = [came[(d + i) * pitch + rows : (d + i + 1) * pitch, :].astype(F32)[:1] for i in range(each)]
        key = ends[0]
        for i in range(1, each):
            key = jnp.where(turn == i, ends[i], key)
        keys.append(key)
    key = jnp.concatenate(keys, axis=1).astype(I32)
    key = (key - 1) * BLOCK + iota((1, groups * BLOCK), 1) % BLOCK
    hot = (iota((total, groups * BLOCK), 0) == key).astype(F32).astype(BF16)

    def strip(first, size):
        return [came[d * pitch + first : d * pitch + first + size, :] for d in range(groups)]

    for j in range(0, full, 2):
        parts = [jnp.concatenate(strip(i * BLOCK, BLOCK), axis=0) for i in range(j, min(j + 2, full))]
        got = jnp.dot(hot, jnp.concatenate(parts, axis=1), preferred_element_type=F32)
        out[:, j * LANES : (j + len(parts)) * LANES] = got.astype(BF16)
    if rows > full * BLOCK:
        twice = jnp.concatenate([x for part in strip(full * BLOCK, BLOCK // 2) for x in (part, part)], axis=0)
        got = jnp.dot(hot, twice, preferred_element_type=F32)
        low = iota((total, LANES), 0) % BLOCK < BLOCK // 2
        left = iota((total, LANES), 1) < HALF
        out[:, full * LANES :] = jnp.where(low == left, got, pltpu.roll(got, HALF, 1)).astype(BF16)


def columns(width, most):
    step = max(d for d in range(LANES, most + 1, LANES) if width % d == 0)
    return [(c, step) for c in range(0, width, step)]


def first_kernel(own, w, out):
    depth = w.shape[0] // 2
    deep = depth // LANES * LANES
    start = pl.multiple_of(lax.axis_index("tensor") * depth, HALF)
    for c, n in columns(out.shape[1], 768):
        out[:, c : c + n] = jnp.dot(own[:, :deep], w[pl.ds(start, deep), c : c + n], preferred_element_type=F32)


def gelu(x):
    inner = x * (GELU_A + GELU_B * (x * x))
    half = 0.5 * x
    return half + half * jnp.tanh(inner)


def hidden_kernel(acc, own, other, w, b, w2, hidden, away, extra):
    me = lax.axis_index("tensor")
    depth = w.shape[0] // 2
    deep = depth // LANES * LANES
    mine = pl.multiple_of(me * depth, HALF)
    theirs = pl.multiple_of((1 - me) * depth, HALF)
    left = other[:, :deep]
    if deep < depth:
        low = iota((other.shape[0], LANES), 1) < HALF
        both = jnp.where(low, own[:, deep:].astype(F32), other[:, deep:].astype(F32)).astype(BF16)
        left = jnp.concatenate([left, both], axis=1)
    for c, n in columns(acc.shape[1], 768):
        right = w[pl.ds(theirs, deep), c : c + n]
        if deep < depth:
            right = jnp.concatenate(
                [right, w[pl.ds(mine + deep, HALF), c : c + n], w[pl.ds(theirs + deep, HALF), c : c + n]], axis=0
            )
        got = jnp.dot(left, right, preferred_element_type=F32)
        got = got + acc[:, c : c + n] + b[:, c : c + n]
        hidden[:, c : c + n] = gelu(got).astype(BF16)
    width = away.shape[1]
    odd = width % TILE
    window = width + odd
    base = (1 - me) * (width - odd)
    ends = []
    for c in range(0, window, TILE):
        col = pl.multiple_of(base + c, LANES)
        got = jnp.dot(hidden[...], w2[:, pl.ds(col, TILE)], preferred_element_type=F32).astype(BF16)
        for h in range(0, TILE, LANES):
            piece = got[:, h : h + LANES]
            if odd and (c + h == 0 or c + h == window - LANES):
                ends.append(piece.astype(F32))
            else:
                at = c + h - LANES * (1 - me) if odd else c + h
                away[:, pl.ds(pl.multiple_of(at, LANES), LANES)] = piece
    if odd:
        at = pl.multiple_of((1 - me) * (width - LANES), LANES)
        away[:, pl.ds(at, LANES)] = jnp.where(me == 0, ends[1], ends[0]).astype(BF16)
        extra[...] = jnp.where(me == 0, ends[0], ends[1]).astype(BF16)


def second_kernel(hidden, w2, extra, part):
    width = part.shape[1]
    odd = width % TILE
    me = lax.axis_index("tensor")
    if odd:
        part[:, pl.ds(pl.multiple_of((1 - me) * (width - odd), LANES), odd)] = extra[...]
    for c in range(0, width - odd, TILE):
        col = pl.multiple_of(me * (width + odd) + c, LANES)
        got = jnp.dot(hidden[...], w2[:, pl.ds(col, TILE)], preferred_element_type=F32).astype(BF16)
        part[:, pl.ds(pl.multiple_of(me * odd + c, LANES), TILE)] = got


def final_kernel(part, back, b, out, held, sems):
    pieces = sems.shape[0]
    rows = out.shape[0] // pieces
    copies = []
    for i in range(pieces):
        at = slice(i * rows, (i + 1) * rows)
        held[at, :] = (part[at, :].astype(F32) + back[at, :].astype(F32) + b[...]).astype(BF16)
        copies.append(pltpu.make_async_copy(held.at[at], out.at[at], sems.at[i]))
        copies[-1].start()
    for copy in copies:
        copy.wait()


def in_hbm(x):
    return pltpu.with_memory_space_constraint(x, pltpu.HBM)


def call(kernel, shapes, specs, out_specs, flops, nbytes, scratch=()):
    return pl.pallas_call(
        kernel,
        out_shape=shapes,
        in_specs=specs,
        out_specs=out_specs,
        scratch_shapes=list(scratch),
        compiler_params=pltpu.CompilerParams(vmem_limit_bytes=GRANT),
        cost_estimate=pl.CostEstimate(flops=int(flops), bytes_accessed=int(nbytes), transcendentals=0),
        name=getattr(kernel, "func", kernel).__name__.removesuffix("_kernel"),
    )


def shards(encoded, counts, win_ids, dest_seq, dest_slot, w_first, b_first, w_second, b_second):
    groups = lax.axis_size("dp")
    samples = counts.shape[0]
    tokens, features = encoded.shape
    units = w_first.shape[1]
    width = b_second.shape[0]
    full, rest, rows = block_rows(features)
    total = samples * BLOCK
    swap = ((0, 1), (1, 0))
    shape = jax.ShapeDtypeStruct
    dma = pltpu.SemaphoreType.DMA
    ints = pltpu.SMEM((samples,), I32)
    lead = groups * 3 // 4 - 1
    ring = [[(lead + i) % groups for i in range(groups)]]

    hot, note, enc = call(
        functools.partial(load_kernel, groups - lead),
        (pltpu.VMEM((groups * BLOCK, tokens), BF16), pltpu.VMEM((groups * NOTE, LANES), BF16), pltpu.VMEM((features, tokens), BF16)),
        [HBM] * 5,
        (VMEM, VMEM, VMEM),
        0,
        2 * tokens * features,
        [ints, ints, ints, pltpu.VMEM(win_ids.shape, I32), dma((4,)), dma],
    )(in_hbm(counts), in_hbm(dest_seq), in_hbm(dest_slot), in_hbm(win_ids), in_hbm(encoded.T))
    outgoing = call(
        pool_kernel,
        shape((groups * (rows + NOTE), LANES), BF16),
        [VMEM] * 3,
        VMEM,
        POOL_FLOPS,
        POOL_BYTES,
    )(hot, note, enc)
    outgoing = outgoing.reshape(groups, -1, NOTE, LANES)
    came = lax.all_to_all(outgoing, "dp", split_axis=0, concat_axis=0, tiled=True, axis_index_groups=ring)
    came = came.reshape(-1, LANES)
    own = call(
        functools.partial(place_kernel, groups=groups),
        shape((total, (full + (rest > 0)) * LANES), BF16),
        [VMEM],
        VMEM,
        2 * total * groups * BLOCK * features,
        4 * total * features,
    )(came)
    other = lax.ppermute(own, "tensor", swap)
    acc = call(
        first_kernel,
        shape((total, units), F32),
        [VMEM] * 2,
        VMEM,
        2 * total * features * units,
        4 * total * units,
    )(own, w_first)
    hidden, away, extra = call(
        hidden_kernel,
        (shape((total, units), BF16), shape((total, width), BF16), shape((total, LANES), BF16)),
        [VMEM] * 6,
        (VMEM, VMEM, VMEM),
        2 * total * (features + width) * units,
        4 * total * units,
    )(acc, own, other, w_first, b_first.reshape(1, -1), w_second)
    back = lax.ppermute(away, "tensor", swap)
    part = call(
        second_kernel,
        shape((total, width), BF16),
        [VMEM] * 3,
        VMEM,
        2 * total * width * units,
        4 * total * units,
    )(hidden, w_second, extra)
    return call(
        final_kernel,
        shape((total, width), BF16),
        [VMEM] * 3,
        ANY,
        total * width,
        4 * total * width,
        [pltpu.VMEM((total, width), BF16), dma((PIECES,))],
    )(part, back, b_second.reshape(1, -1))


def solution(mesh):
    placed = (
        P("dp", "tensor"),
        P("dp"),
        P("dp", None),
        P("dp"),
        P("dp"),
        P(None, "tensor"),
        P("tensor"),
        P("tensor", None),
        P("tensor"),
    )
    return jax.shard_map(
        shards, mesh=mesh, in_specs=placed, out_specs=P("dp", "tensor"), check_vma=False
    )
```
